32 devices in a mesh: rep: 4 (over x, core), shard: 8 (over z, y).
Axes of the slice: x: 2, y: 2, z: 4, core: 2. Of those that a mesh axis runs over, the one named last changes fastest.
Arguments:
- dense_out: bfloat16 [4096, 128], P(('rep', 'shard')), may hold values from -0.75 to 0.75
- pooled: bfloat16 [4096, 26, 128], P(('rep', 'shard')), may hold values from -0.75 to 0.75
- top_weight: bfloat16 [479, 1024], replicated, may hold values from -0.25 to 0.25
- top_cotangent: bfloat16 [4096, 1024], P(('rep', 'shard')), may hold values from -3 to 3
- indices: int32 [4096, 26, 2], P(('rep', 'shard')), may hold values from 0 to 2047, as said below
Outputs:
- dense_grad: bfloat16 [4096, 128], P(('rep', 'shard'))
- top_grad: float32 [479, 1024], replicated
- bias_grad: float32 [1024], replicated
- table_grad: float32 [26, 2048, 128], P(None, 'shard')
The draws below stay inside these ranges and needn't reach their ends.
Inputs may be any that keep to these rules, and one draw needn't show every extreme that they name: `indices`: rows r with r // 256 = s are held by shard s. For every device's 128 samples and every table, at most 16 of the device's lookups fall in any one block of 64 rows starting at a multiple of 64, and some such block holds exactly 16.
All inputs are finite; a program needn't handle non-finite values.
Results may differ from the reference program's by a relative error of at most 0.008.
Values may be sent and summed in bfloat16 or wider, within the bound.
No kernel may reach another device: no remote copies, remote signals or barrier semaphores. Data moves between devices by JAX's collectives and lax.ppermute only.
A program may use at most 128 MiB of HBM per device.

```python
import jax
import jax.numpy as jnp
import numpy as np
from jax import lax

E = 128
F = 26
H = 1024
B_DEV = 128
L = 2
R_SHARD = 256
IN = 479
BATCH = 4096
ROWS = 2048
N_REP = 4
N_SHARD = 8


def draw_indices(key, part):
    devices_all = N_REP * N_SHARD
    blocks = N_SHARD * N_REP
    per_block = 2 * B_DEV * L // blocks
    lookups = B_DEV * L
    row_span = R_SHARD // N_REP
    places = blocks * per_block

    def draw_bag(subkey):
        key_full, key_order, key_offset, key_shuffle = jax.random.split(subkey, 4)
        full_block = jax.random.randint(key_full, (), 0, blocks, dtype=jnp.int32)
        place_ids = jnp.arange(places, dtype=jnp.int32)
        ranking = jax.random.permutation(key_order, places).astype(jnp.int32)
        scores = jnp.where(place_ids // per_block == full_block, place_ids - places, ranking)
        chosen = jnp.argsort(scores, stable=True)[:lookups].astype(jnp.int32)
        offsets = jax.random.randint(key_offset, (lookups,), 0, row_span, dtype=jnp.int32)
        rows_drawn = chosen // per_block * row_span + offsets
        shuffle = jax.random.permutation(key_shuffle, lookups)
        return rows_drawn[shuffle].reshape(B_DEV, L)
    subkeys = jax.random.split(key, devices_all * F)
    drawn_rows = jax.vmap(draw_bag)(subkeys).reshape(devices_all, F, B_DEV, L)
    return jnp.transpose(drawn_rows, (0, 2, 1, 3)).reshape(devices_all * B_DEV, F, L).astype(jnp.int32)


def steps_of(rng, extent, shards, smallest, high):
    factor_of, own = 1.0, jax.random.fold_in(rng, 6)
    for position, blocks in shards:
        draws = jnp.exp(jax.random.uniform(jax.random.fold_in(own, position), (blocks,), jnp.float32, smallest / len(shards), high / len(shards)))
        factor_of = factor_of * jnp.repeat(draws, extent[position] // blocks).reshape([-1 if axis == position else 1 for axis in range(len(extent))])
    return factor_of


def bell_draw(rng, shape, deviation, bound, pieces=(), held_as=jnp.bfloat16):
    factor_of = steps_of(rng, shape, pieces, -0.22, 0.18) if pieces else 1.0
    array = jax.random.normal(rng, shape, jnp.float32) * deviation * factor_of
    return jnp.minimum(jnp.maximum(array, -bound), bound).astype(held_as)


def setup_inputs(seed: int = 0) -> dict:
    keys = jax.random.split(jax.random.key(seed), 6)
    return {
        "dense_out": bell_draw(keys[0], (BATCH, E), 0.125, 0.75, ((0, 32),)),
        "pooled": bell_draw(keys[1], (BATCH, F, E), 0.125, 0.75, ((0, 32),)),
        "top_weight": bell_draw(keys[2], (IN, H), IN ** -0.5, 0.25),
        "top_cotangent": bell_draw(keys[3], (BATCH, H), 0.5, 3.0, ((0, 32),)),
        "indices": draw_indices(jax.random.fold_in(keys[5], 71), 0),
    }


highest = lax.Precision.HIGHEST


def reference(dense_out, pooled, top_weight, top_cotangent, indices):
    vectors = F + 1
    lower_i, lower_j = np.tril_indices(vectors, -1)
    blocks = BATCH // B_DEV
    table_index = jnp.arange(F, dtype=jnp.int32)

    def block_step(totals, inputs):
        top_acc, bias_acc, table_acc = totals
        dense_block, pooled_block, cot_block, index_block = inputs
        stacked = jnp.concatenate([dense_block[:, None, :], pooled_block], axis=1).astype(jnp.float32)
        gram_matrix = jnp.einsum("bie,bje->bij", stacked, stacked, precision=highest)
        pair_values = gram_matrix[:, lower_i, lower_j].astype(jnp.bfloat16)
        joined = jnp.concatenate([dense_block, pair_values], axis=1)
        grad_in = jnp.dot(cot_block, top_weight.T, preferred_element_type=jnp.float32)
        top_acc = top_acc + jnp.dot(joined.T, cot_block, preferred_element_type=jnp.float32)
        bias_acc = bias_acc + jnp.sum(cot_block.astype(jnp.float32), axis=0)
        pair_grad = grad_in[:, E:]
        mirror = jnp.zeros((pair_grad.shape[0], vectors, vectors), jnp.float32)
        mirror = mirror.at[:, lower_i, lower_j].set(pair_grad)
        mirror = mirror.at[:, lower_j, lower_i].set(pair_grad)
        vec_grad = jnp.einsum("bij,bje->bie", mirror, stacked, precision=highest)
        dense_grad = (grad_in[:, :E] + vec_grad[:, 0]).astype(jnp.bfloat16)
        pooled_grad = vec_grad[:, 1:].astype(jnp.bfloat16)
        updates = jnp.broadcast_to(pooled_grad.astype(jnp.float32)[:, :, None, :], (B_DEV, F, L, E))
        table_acc = table_acc.at[table_index[None, :, None], index_block].add(updates)
        return (top_acc, bias_acc, table_acc), dense_grad

    start = (jnp.zeros((IN, H), jnp.float32), jnp.zeros((H,), jnp.float32), jnp.zeros((F, ROWS, E), jnp.float32))
    inputs = (dense_out.reshape(blocks, B_DEV, E), pooled.reshape(blocks, B_DEV, F, E), top_cotangent.reshape(blocks, B_DEV, H), indices.reshape(blocks, B_DEV, F, L))
    totals, dense_parts = lax.scan(block_step, start, inputs)
    top_grad, bias_grad, table_grad = totals
    return dense_parts.reshape(BATCH, E), top_grad, bias_grad, table_grad
```

```python
import functools

import jax
import jax.numpy as jnp
import numpy as np
from jax import lax
from jax.experimental import pallas as pl
from jax.experimental.pallas import tpu as pltpu
from jax.sharding import PartitionSpec as P

R_SHARD = 256
KEY_TILE = 8


def pair_tables(vectors):
    lower_i, lower_j = np.tril_indices(vectors, -1)
    pairs = lower_i.shape[0]
    select = np.zeros((vectors * vectors, pairs), np.float32)
    select[lower_i * vectors + lower_j, np.arange(pairs)] = 1.0
    mirrored = np.zeros((pairs, vectors * vectors), np.float32)
    mirrored[np.arange(pairs), lower_i * vectors + lower_j] = 1.0
    mirrored[np.arange(pairs), lower_j * vectors + lower_i] = 1.0
    return (jnp.asarray(select, jnp.bfloat16), jnp.asarray(mirrored, jnp.bfloat16))


def sums_kernel(sources, dest_ref, *refs):
    row_refs, plane_refs = refs[:sources], refs[sources : 2 * sources]
    out_ref, keys_ref = refs[2 * sources :]
    lookups = keys_ref.shape[0]
    table = pl.program_id(0)
    slot = pl.program_id(1)

    @pl.when((table == 0) & (slot == 0))
    def _():
        for k in range(sources):
            planes = plane_refs[k][...].astype(jnp.float32)
            for l in range(lookups):
                base = 2 * l * KEY_TILE
                owner = planes[base : base + KEY_TILE]
                row = planes[base + KEY_TILE : base + 2 * KEY_TILE]
                keys_ref[l, k] = owner * R_SHARD + row

    height = out_ref.shape[2]
    samples = row_refs[0].shape[0]
    start = (dest_ref[slot] * R_SHARD).astype(jnp.float32)
    level = lax.broadcasted_iota(jnp.int32, (height, samples), 0).astype(jnp.float32)
    offset = dest_ref[dest_ref.shape[0] - 1] + table
    hots = []
    for k in range(sources):
        hot = None
        for l in range(lookups):
            key = keys_ref[l, k, pl.ds(offset, 1), :] - start
            one = jnp.where(level == key, 1.0, 0.0)
            hot = one if hot is None else hot + one
        hots.append(hot.astype(jnp.bfloat16))
    rows = jnp.concatenate([ref[...] for ref in row_refs], axis=0)
    total = jnp.dot(jnp.concatenate(hots, axis=1), rows, preferred_element_type=jnp.float32)
    out_ref[0, 0] = total.astype(out_ref.dtype)


def row_sums(payloads, dests, first, count, per_group, samples, lookups, out_dtype):
    sources = len(payloads)
    width = payloads[0].shape[1]
    plane_rows = 2 * lookups * KEY_TILE
    slots = dests.shape[0]
    last = per_group * samples // plane_rows
    scalars = jnp.concatenate([dests, jnp.full((1,), first, jnp.int32)])
    return pl.pallas_call(
        functools.partial(sums_kernel, sources),
        grid_spec=pltpu.PrefetchScalarGridSpec(
            num_scalar_prefetch=1,
            grid=(count, slots),
            in_specs=[pl.BlockSpec((samples, width), lambda t, j, s: (t + first, 0))] * sources
            + [pl.BlockSpec((plane_rows, width), lambda t, j, s: (last, 0))] * sources,
            out_specs=pl.BlockSpec((1, 1, R_SHARD, width), lambda t, j, s: (j, t, 0, 0)),
            scratch_shapes=[pltpu.VMEM((lookups, sources, KEY_TILE, width), jnp.float32)],
        ),
        out_shape=jax.ShapeDtypeStruct((slots, count, R_SHARD, width), out_dtype),
        cost_estimate=pl.CostEstimate(
            flops=8 * count * slots * R_SHARD * sources * samples * width,
            bytes_accessed=4 * count * slots * R_SHARD * width,
            transcendentals=0,
        ),
        name="row_sums",
    )(scalars, *payloads, *payloads)


def on_device(dense_out, pooled, top_weight, top_cotangent, indices):
    samples, emb_width = dense_out.shape
    tables = pooled.shape[1]
    lookups = indices.shape[2]
    replicas = lax.axis_size("rep")
    shards = lax.axis_size("shard")
    vectors = tables + 1
    select, mirrored = pair_tables(vectors)
    rep = lax.axis_index("rep")

    stacked = jnp.concatenate([dense_out[:, None, :], pooled], axis=1)
    grad_in = lax.dot_general(
        top_cotangent, top_weight, (((1,), (1,)), ((), ())), preferred_element_type=jnp.float32
    )
    pair_grad = grad_in[:, emb_width:].astype(jnp.bfloat16)
    mirror = (
        jnp.dot(pair_grad, mirrored, preferred_element_type=jnp.float32)
        .astype(jnp.bfloat16)
        .reshape(samples, vectors, vectors)
    )
    vec_grad = jnp.einsum("bij,bje->bie", mirror, stacked, preferred_element_type=jnp.float32)
    dense_grad = (grad_in[:, :emb_width] + vec_grad[:, 0]).astype(jnp.bfloat16)
    pooled_grad = jnp.transpose(vec_grad[:, 1:].astype(jnp.bfloat16), (1, 0, 2))

    group = -(-tables // replicas)
    shard = lax.axis_index("shard").astype(jnp.int32)

    def swap(array, axis, bit):
        size = lax.axis_size(axis)
        return lax.ppermute(array, axis, [(i, i ^ bit) for i in range(size)])

    def bits_of(size):
        return [1 << n for n in range(size.bit_length() - 1)]

    by_table = jnp.transpose(indices, (2, 1, 0))
    owner = (by_table // R_SHARD).astype(jnp.bfloat16)
    row = (by_table % R_SHARD).astype(jnp.bfloat16)
    planes = jnp.stack([owner, row], axis=1)
    spare = group * replicas - tables
    planes = jnp.pad(planes, ((0, 0), (0, 0), (0, spare), (0, 0)))
    pooled_grad = jnp.pad(pooled_grad, ((0, spare), (0, 0), (0, 0)))

    def payload(which):
        grads = lax.dynamic_slice_in_dim(pooled_grad, which * group, group, 0)
        keys = lax.dynamic_slice_in_dim(planes, which * group, group, 2)
        keys = jnp.pad(keys, ((0, 0), (0, 0), (0, KEY_TILE - group), (0, 0)))
        return jnp.concatenate(
            [grads.reshape(group * samples, emb_width), keys.reshape(-1, samples)], axis=0
        )

    payloads = [payload(rep)] + [
        swap(payload(rep ^ k), "rep", k) for k in range(1, replicas)
    ]

    gram = jnp.einsum("bie,bje->bij", stacked, stacked, preferred_element_type=jnp.float32)
    pair_values = jnp.dot(
        gram.astype(jnp.bfloat16).reshape(samples, vectors * vectors),
        select,
        preferred_element_type=jnp.float32,
    ).astype(jnp.bfloat16)
    used = emb_width + pair_values.shape[1] + 1
    unit = max(512, replicas * shards)
    wide = -(-used // unit) * unit
    joined = jnp.concatenate(
        [
            dense_out,
            pair_values,
            jnp.ones((samples, 1), jnp.bfloat16),
            jnp.zeros((samples, wide - used), jnp.bfloat16),
        ],
        axis=1,
    )
    top = lax.dot_general(
        joined, top_cotangent, (((0,), (0,)), ((), ())), preferred_element_type=jnp.float32
    )
    steps = [("rep", b, rep) for b in bits_of(replicas)]
    steps += [("shard", b, shard) for b in bits_of(shards)]
    for axis, bit, index in steps:
        side = (index // bit) % 2
        rows = top.shape[0] // 2
        sent = lax.dynamic_slice_in_dim(top, (1 - side) * rows, rows, 0).astype(jnp.bfloat16)
        kept = lax.dynamic_slice_in_dim(top, side * rows, rows, 0)
        top = kept + swap(sent, axis, bit).astype(jnp.float32)
    top = top.astype(jnp.bfloat16)
    for axis, bit, index in reversed(steps):
        side = (index // bit) % 2
        other = swap(top, axis, bit)
        top = jnp.where(
            side == 0,
            jnp.concatenate([top, other], axis=0),
            jnp.concatenate([other, top], axis=0),
        )
    top_grad = top[: used - 1].astype(jnp.float32)
    bias_grad = top[used - 1].astype(jnp.float32)

    def scatter(first, count, order):
        far = [j for j in range(shards) if j & order[0]]
        near = [j for j in range(shards) if not j & order[0]]

        def sums(which, dtype):
            dests = shard ^ jnp.asarray(which, jnp.int32)
            return row_sums(payloads, dests, first, count, group, samples, lookups, dtype)

        arrived = swap(sums(far, jnp.bfloat16), "shard", order[0])
        total = sums(near, jnp.float32) + arrived.astype(jnp.float32)
        for bit in order[1:]:
            sent = jnp.stack([total[n] for n, j in enumerate(near) if j & bit])
            kept = jnp.stack([total[n] for n, j in enumerate(near) if not j & bit])
            near = [j for j in near if not j & bit]
            total = kept + swap(sent.astype(jnp.bfloat16), "shard", bit).astype(jnp.float32)
        return total[0].astype(jnp.bfloat16)

    order = bits_of(shards)
    other_order = order[:2][::-1] + order[2:]
    cut = (group + 1) // 2
    mine = jnp.concatenate(
        [scatter(0, cut, order), scatter(cut, group - cut, other_order)], axis=0
    )
    parts = {0: mine}
    for bit in reversed(bits_of(replicas)):
        parts.update({k | bit: swap(part, "rep", bit) for k, part in list(parts.items())})
    for bit in bits_of(replicas):
        flip = (rep // bit) % 2 == 1
        parts = {k: jnp.where(flip, parts[k ^ bit], parts[k]) for k in parts}
    table_grad = jnp.concatenate([parts[k] for k in range(replicas)], axis=0)
    table_grad = table_grad[:tables].astype(jnp.float32)
    return (dense_grad, top_grad, bias_grad, table_grad)


def solution(mesh):
    return jax.shard_map(
        on_device,
        mesh=mesh,
        in_specs=(
            P(("rep", "shard"), None),
            P(("rep", "shard"), None, None),
            P(),
            P(("rep", "shard"), None),
            P(("rep", "shard"), None, None),
        ),
        out_specs=(P(("rep", "shard"), None), P(), P(), P(None, "shard", None)),
        check_vma=False,
    )
```

```python
import functools

import jax
import jax.numpy as jnp
import numpy as np
from jax import lax
from jax.experimental import pallas as pl
from jax.experimental.pallas import tpu as pltpu
from jax.sharding import PartitionSpec as P

R_SHARD = 256
KEY_TILE = 8


def pair_tables(vectors):
    lower_i, lower_j = np.tril_indices(vectors, -1)
    pairs = lower_i.shape[0]
    select = np.zeros((vectors * vectors, pairs), np.float32)
    select[lower_i * vectors + lower_j, np.arange(pairs)] = 1.0
    mirrored = np.zeros((pairs, vectors * vectors), np.float32)
    mirrored[np.arange(pairs), lower_i * vectors + lower_j] = 1.0
    mirrored[np.arange(pairs), lower_j * vectors + lower_i] = 1.0
    return (jnp.asarray(select, jnp.bfloat16), jnp.asarray(mirrored, jnp.bfloat16))


def sums_kernel(sources, first, dest_ref, *refs):
    row_refs, plane_refs = refs[:sources], refs[sources : 2 * sources]
    out_ref, owner_ref, row_ref = refs[2 * sources :]
    lookups = owner_ref.shape[0]
    slots, height = out_ref.shape[0], out_ref.shape[2]
    samples = row_refs[0].shape[0]
    table = pl.program_id(0)

    @pl.when(table == 0)
    def _():
        for k in range(sources):
            planes = plane_refs[k][...].astype(jnp.float32)
            for l in range(lookups):
                base = 2 * l * KEY_TILE
                owner_ref[l, k] = planes[base : base + KEY_TILE]
                row_ref[l, k] = planes[base + KEY_TILE : base + 2 * KEY_TILE]

    level = lax.broadcasted_iota(jnp.int32, (height, samples), 0)
    level = level.astype(jnp.float32).astype(jnp.bfloat16)
    rows = jnp.concatenate([ref[...] for ref in row_refs], axis=0)
    one, zero = jnp.bfloat16(1.0), jnp.bfloat16(0.0)
    at = pl.ds(first + table, 1)

    def fill(slot):
        dest = dest_ref[slot].astype(jnp.float32)
        hots = []
        for k in range(sources):
            hot = None
            for l in range(lookups):
                key = jnp.where(owner_ref[l, k, at, :] == dest, row_ref[l, k, at, :], -1.0)
                key = jnp.broadcast_to(key.astype(jnp.bfloat16), (height, samples))
                match = jnp.where(level == key, one, zero)
                hot = match if hot is None else hot + match
            hots.append(hot)
        hot = jnp.concatenate(hots, axis=1)
        total = jnp.dot(hot, rows, preferred_element_type=jnp.float32)
        out_ref[slot, 0] = total.astype(out_ref.dtype)

    if slots <= 8:
        for slot in range(slots):
            fill(slot)
    else:
        pl.loop(0, slots)(fill)


def row_sums(payloads, dests, first, count, per_group, samples, lookups, out_dtype):
    sources = len(payloads)
    width = payloads[0].shape[1]
    plane_rows = 2 * lookups * KEY_TILE
    slots = dests.shape[0]
    last = per_group * samples // plane_rows
    return pl.pallas_call(
        functools.partial(sums_kernel, sources, first),
        grid_spec=pltpu.PrefetchScalarGridSpec(
            num_scalar_prefetch=1,
            grid=(count,),
            in_specs=[pl.BlockSpec((samples, width), lambda t, s: (t + first, 0))] * sources
            + [pl.BlockSpec((plane_rows, width), lambda t, s: (last, 0))] * sources,
            out_specs=pl.BlockSpec((slots, 1, R_SHARD, width), lambda t, s: (0, t, 0, 0)),
            scratch_shapes=[pltpu.VMEM((lookups, sources, KEY_TILE, width), jnp.float32)] * 2,
        ),
        out_shape=jax.ShapeDtypeStruct((slots, count, R_SHARD, width), out_dtype),
        cost_estimate=pl.CostEstimate(
            flops=8 * count * slots * R_SHARD * sources * samples * width,
            bytes_accessed=4 * count * slots * R_SHARD * width,
            transcendentals=0,
        ),
        name="row_sums",
    )(dests, *payloads, *payloads)


def on_device(dense_out, pooled, top_weight, top_cotangent, indices):
    samples, emb_width = dense_out.shape
    tables = pooled.shape[1]
    lookups = indices.shape[2]
    replicas = lax.axis_size("rep")
    shards = lax.axis_size("shard")
    vectors = tables + 1
    select, mirrored = pair_tables(vectors)
    rep = lax.axis_index("rep")

    stacked = jnp.concatenate([dense_out[:, None, :], pooled], axis=1)
    grad_in = lax.dot_general(
        top_cotangent, top_weight, (((1,), (1,)), ((), ())), preferred_element_type=jnp.float32
    )
    pair_grad = grad_in[:, emb_width:].astype(jnp.bfloat16)
    mirror = (
        jnp.dot(pair_grad, mirrored, preferred_element_type=jnp.float32)
        .astype(jnp.bfloat16)
        .reshape(samples, vectors, vectors)
    )
    vec_grad = jnp.einsum("bij,bje->bie", mirror, stacked, preferred_element_type=jnp.float32)
    dense_grad = (grad_in[:, :emb_width] + vec_grad[:, 0]).astype(jnp.bfloat16)
    pooled_grad = jnp.transpose(vec_grad[:, 1:].astype(jnp.bfloat16), (1, 0, 2))

    group = -(-tables // replicas)
    shard = lax.axis_index("shard").astype(jnp.int32)

    def swap(array, axis, bit):
        size = lax.axis_size(axis)
        return lax.ppermute(array, axis, [(i, i ^ bit) for i in range(size)])

    def bits_of(size):
        return [1 << n for n in range(size.bit_length() - 1)]

    by_table = jnp.transpose(indices, (2, 1, 0))
    owner = (by_table // R_SHARD).astype(jnp.bfloat16)
    row = (by_table % R_SHARD).astype(jnp.bfloat16)
    planes = jnp.stack([owner, row], axis=1)
    spare = group * replicas - tables
    planes = jnp.pad(planes, ((0, 0), (0, 0), (0, spare), (0, 0)))
    pooled_grad = jnp.pad(pooled_grad, ((0, spare), (0, 0), (0, 0)))

    def payload(which):
        grads = lax.dynamic_slice_in_dim(pooled_grad, which * group, group, 0)
        keys = lax.dynamic_slice_in_dim(planes, which * group, group, 2)
        keys = jnp.pad(keys, ((0, 0), (0, 0), (0, KEY_TILE - group), (0, 0)))
        return jnp.concatenate(
            [grads.reshape(group * samples, emb_width), keys.reshape(-1, samples)], axis=0
        )

    payloads = [payload(rep)] + [
        swap(payload(rep ^ k), "rep", k) for k in range(1, replicas)
    ]

    gram = jnp.einsum("bie,bje->bij", stacked, stacked, preferred_element_type=jnp.float32)
    pair_values = jnp.dot(
        gram.astype(jnp.bfloat16).reshape(samples, vectors * vectors),
        select,
        preferred_element_type=jnp.float32,
    ).astype(jnp.bfloat16)
    used = emb_width + pair_values.shape[1] + 1
    unit = max(512, replicas * shards)
    wide = -(-used // unit) * unit
    joined = jnp.concatenate(
        [
            dense_out,
            pair_values,
            jnp.ones((samples, 1), jnp.bfloat16),
            jnp.zeros((samples, wide - used), jnp.bfloat16),
        ],
        axis=1,
    )
    top = lax.dot_general(
        joined, top_cotangent, (((0,), (0,)), ((), ())), preferred_element_type=jnp.float32
    )
    steps = [("rep", b, rep) for b in bits_of(replicas)]
    steps += [("shard", b, shard) for b in bits_of(shards)]

    def after(array, *others):
        return lax.optimization_barrier((array, others))[0]

    def halve(axis, bit, index, *others):
        nonlocal top
        side = (index // bit) % 2
        rows = top.shape[0] // 2
        sent = lax.dynamic_slice_in_dim(top, (1 - side) * rows, rows, 0).astype(jnp.bfloat16)
        kept = lax.dynamic_slice_in_dim(top, side * rows, rows, 0)
        arrived = swap(sent, axis, bit)
        top = after(kept, *others) + after(arrived, *others).astype(jnp.float32)

    def hop(bit):
        return bit | (bit >> 1) if bit >= 4 else bit

    def apart(slot):
        return functools.reduce(lambda j, b: j ^ hop(b) if slot & b else j, order, 0)

    def sums(span, which, dtype):
        dests = shard ^ jnp.asarray([apart(q) for q in which], jnp.int32)
        first, count = span
        return row_sums(payloads, dests, first, count, group, samples, lookups, dtype)

    order = bits_of(shards)
    orders = [order, order[:2][::-1] + order[2:]]
    cut = (group + 1) // 2
    spans = [(0, cut), (cut, group - cut)]
    fars = [[j for j in range(shards) if j & o[0]] for o in orders]
    nears = [[j for j in range(shards) if not j & o[0]] for o in orders]
    away = [sums(p, w, jnp.bfloat16) for p, w in zip(spans, fars)]
    arrived = [swap(x, "shard", hop(o[0])) for x, o in zip(away, orders)]
    held = [sums(p, w, jnp.float32) for p, w in zip(spans, nears)]
    for n, step in enumerate(steps[: len(bits_of(replicas))]):
        halve(*step, *(away if n == 0 else held))
    totals = [h + x.astype(jnp.float32) for h, x in zip(held, arrived)]
    for turn, step in enumerate(steps[len(bits_of(replicas)) :], 1):
        if turn < len(order):
            sent, kept = [], []
            for c in range(2):
                bit, near = orders[c][turn], nears[c]
                out = jnp.stack([totals[c][n] for n, j in enumerate(near) if j & bit])
                sent.append(out.astype(jnp.bfloat16))
                kept.append(jnp.stack([totals[c][n] for n, j in enumerate(near) if not j & bit]))
                nears[c] = [j for j in near if not j & bit]
            arrived = [swap(x, "shard", hop(o[turn])) for x, o in zip(sent, orders)]
            halve(*step, *sent)
            totals = [k + x.astype(jnp.float32) for k, x in zip(kept, arrived)]
        else:
            mine = [t[0].astype(jnp.bfloat16) for t in totals]
            halve(*step)
    top = top.astype(jnp.bfloat16)
    for axis, bit, index in reversed(steps):
        side = (index // bit) % 2
        other = swap(top, axis, bit)
        top = jnp.where(
            side == 0,
            jnp.concatenate([top, other], axis=0),
            jnp.concatenate([other, top], axis=0),
        )
    top_grad = top[: used - 1].astype(jnp.float32)
    bias_grad = top[used - 1].astype(jnp.float32)

    def spread(part):
        parts = {0: part}
        for bit in reversed(bits_of(replicas)):
            parts.update({k | bit: swap(p, "rep", bit) for k, p in list(parts.items())})
        return parts

    upper, lower = [spread(m) for m in mine]
    parts = {k: jnp.concatenate([upper[k], lower[k]], axis=0) for k in upper}
    for bit in bits_of(replicas):
        flip = (rep // bit) % 2 == 1
        parts = {k: jnp.where(flip, parts[k ^ bit], parts[k]) for k in parts}
    table_grad = jnp.concatenate([parts[k] for k in range(replicas)], axis=0)
    table_grad = table_grad[:tables].astype(jnp.float32)
    return (dense_grad, top_grad, bias_grad, table_grad)


def solution(mesh):
    return jax.shard_map(
        on_device,
        mesh=mesh,
        in_specs=(
            P(("rep", "shard"), None),
            P(("rep", "shard"), None, None),
            P(),
            P(("rep", "shard"), None),
            P(("rep", "shard"), None, None),
        ),
        out_specs=(P(("rep", "shard"), None), P(), P(), P(None, "shard", None)),
        check_vma=False,
    )
```
